16 devices in a mesh: rep: 2 (over y, z), dp: 8 (over x, core).
Axes of the slice: x: 4, y: 2, z: 1, core: 2. Of those that a mesh axis runs over, the one named last changes fastest.
The devices are a block of a 4x4x8 slice.
Arguments:
- x: bfloat16 [16, 2048, 1024], P(('rep', 'dp')), parts along dimension 0
- dy: bfloat16 [16, 2048, 1024], P(('rep', 'dp')), parts along dimension 0
- w_gate: bfloat16 [2, 1024, 3200], P(None, 'dp')
- w_up: bfloat16 [2, 1024, 3200], P(None, 'dp')
- w_down: bfloat16 [2, 3200, 1024], P(None, 'dp')
- m_w_gate: float32 [2, 1024, 3200], P(None, 'dp')
- m_w_up: float32 [2, 1024, 3200], P(None, 'dp')
- m_w_down: float32 [2, 3200, 1024], P(None, 'dp')
- v_w_gate: float32 [2, 1024, 3200], P(None, 'dp')
- v_w_up: float32 [2, 1024, 3200], P(None, 'dp')
- v_w_down: float32 [2, 3200, 1024], P(None, 'dp')
Outputs:
- output 1: bfloat16 [4, 1024, 3200], P('rep', 'dp'), parts along dimension 0
- output 2: bfloat16 [4, 1024, 3200], P('rep', 'dp'), parts along dimension 0
- output 3: bfloat16 [4, 3200, 1024], P('rep', 'dp'), parts along dimension 0
- output 4: float32 [4, 1024, 3200], P('rep', 'dp'), parts along dimension 0
- output 5: float32 [4, 1024, 3200], P('rep', 'dp'), parts along dimension 0
- output 6: float32 [4, 3200, 1024], P('rep', 'dp'), parts along dimension 0
- output 7: float32 [4, 1024, 3200], P('rep', 'dp'), parts along dimension 0
- output 8: float32 [4, 1024, 3200], P('rep', 'dp'), parts along dimension 0
- output 9: float32 [4, 3200, 1024], P('rep', 'dp'), parts along dimension 0
There are 2 independent parts. The reference program is written for one: setup_inputs(seed, part) draws one part's arguments, and reference() takes and returns one part's arrays. A program takes and returns all parts, laid end to end along the dimension named above; an argument that names none is the same for every part.
All inputs are finite; a program needn't handle non-finite values.
Results may differ from the reference program's by a relative error of at most 0.0237.
Values are sent between devices in bfloat16 or wider.
A program may use at most 768 MiB of HBM per device.

```python
import jax
import jax.numpy as jnp
from jax import lax

SEQUENCES = 8
TOKENS = 2048
D = 1024
FF = 3200
LAYERS = 2
NAMES = ("w_gate", "w_up", "w_down")
SHAPES = {"w_gate": (LAYERS, D, FF), "w_up": (LAYERS, D, FF), "w_down": (LAYERS, FF, D)}


def bump(key, n, height):
    away = (jnp.arange(n, dtype=jnp.int32) - jax.random.randint(key, (), 0, n, jnp.int32)) % n
    return jnp.where(away < n // 8, height, 1.0)


def together(key, own, strength):
    shared = jax.random.normal(key, own.shape[1:], jnp.float32)
    return (own + strength * shared) * lax.rsqrt(1 + strength * strength)


def setup_inputs(seed: int = 0, part: int = 0) -> dict:
    kx, kdy, ka, kb, kz, kf, kh, kl, *keys = jax.random.split(jax.random.key(seed), 8 + 3 * len(NAMES))
    kx, kdy, ka, kb = (jax.random.fold_in(k, part) for k in (kx, kdy, ka, kb))
    kw, km, kv = (keys[i::3] for i in range(3))
    shape = (SEQUENCES, TOKENS, D)
    much_x, much_dy = jax.random.uniform(kz, (2,), jnp.float32, 0.0, 1.0)
    loud = 2.0 ** jax.random.uniform(jax.random.fold_in(kz, 1), (), jnp.float32, -1.0, 2.0)
    layers = 2.0 ** jax.random.uniform(kl, (LAYERS, 1, 1), jnp.float32, -1.0, 1.0)
    x = together(ka, jax.random.normal(kx, shape, jnp.float32), much_x) * bump(kf, D, 4.0)
    dy = together(kb, jax.random.normal(kdy, shape, jnp.float32), much_dy)
    drawn = {"x": x.astype(jnp.bfloat16), "dy": (loud * dy * (SEQUENCES * TOKENS) ** -0.5).astype(jnp.bfloat16)}
    for key, name in zip(kw, NAMES, strict=True):
        w = jax.random.normal(key, SHAPES[name], jnp.float32) * SHAPES[name][1] ** -0.5
        drawn[name] = (w * {"w_gate": 1.0, "w_up": bump(kh, FF, 4.0), "w_down": layers}[name]).astype(jnp.bfloat16)
    for key, name in zip(km, NAMES, strict=True):
        drawn[f"m_{name}"] = 0.1 * jax.random.normal(key, SHAPES[name], jnp.float32)
    for key, name in zip(kv, NAMES, strict=True):
        drawn[f"v_{name}"] = jax.random.uniform(key, SHAPES[name], jnp.float32, 0.005, 0.015)
    return drawn


def matmul(a, w):
    return jnp.dot(a, w, preferred_element_type=jnp.float32).astype(jnp.bfloat16)


def normed(h):
    wide = h.astype(jnp.float32)
    scale = lax.rsqrt(jnp.mean(wide**2, -1, keepdims=True) + 1e-6)
    return (wide * scale).astype(jnp.bfloat16)


def layer(h, w):
    a = normed(h)
    gate = jnp.dot(a, w["w_gate"], preferred_element_type=jnp.float32)
    up = jnp.dot(a, w["w_up"], preferred_element_type=jnp.float32)
    return h + matmul((jax.nn.silu(gate) * up).astype(jnp.bfloat16), w["w_down"])


def adamw(w, m, v, g):
    m = 0.9 * m + 0.1 * g
    v = 0.95 * v + 0.05 * g * g
    step = m * lax.rsqrt(v + 1e-8) + 0.1 * w
    return (w - 0.02 * step).astype(jnp.bfloat16), m, v


def stack(weights, h):
    return lax.scan(lambda h, w: (layer(h, w), None), h, weights)[0]


def reference(x, dy, w_gate, w_up, w_down, m_w_gate, m_w_up, m_w_down, v_w_gate, v_w_up, v_w_down):
    weights = dict(zip(NAMES, (w_gate, w_up, w_down), strict=True))

    def take(so_far, sequence):
        h, by_y = sequence
        _, back = jax.vjp(lambda w: stack(w, h), weights)
        return jax.tree.map(lambda total, term: total + term.astype(jnp.float32), so_far, back(by_y)[0]), None

    none_yet = {name: jnp.zeros(w.shape, jnp.float32) for name, w in weights.items()}
    by_weights, _ = lax.scan(take, none_yet, (x, dy))
    gradients = [by_weights[name].astype(jnp.bfloat16).astype(jnp.float32) for name in NAMES]
    new = [
        adamw(w.astype(jnp.float32), m, v, g)
        for w, m, v, g in zip((w_gate, w_up, w_down), (m_w_gate, m_w_up, m_w_down), (v_w_gate, v_w_up, v_w_down), gradients, strict=True)
    ]
    return tuple(one[which] for which in range(3) for one in new)
```

```python
import functools

import jax
import jax.numpy as jnp
from jax import lax
from jax.experimental import pallas as pl
from jax.experimental.pallas import tpu as pltpu
from jax.sharding import PartitionSpec as P

MESH = pl.DeviceIdType.MESH
F32, BF16 = jnp.float32, jnp.bfloat16
ANY = pl.BlockSpec(memory_space=pl.ANY)
BM = 256
MB = 2**20


def dot(a, b, ca=1, cb=0):
    return lax.dot_general(a, b, (((ca,), (cb,)), ((), ())), preferred_element_type=F32)


def normed(wide):
    scale = lax.rsqrt(jnp.mean(wide * wide, -1, keepdims=True) + 1e-6)
    return (wide * scale).astype(BF16)


def thirds(n, unit):
    tiles = n // unit
    side = tiles // 3
    return side * unit, (tiles - 2 * side) * unit, side * unit


def cuts(n):
    k = max(1, n // 512)
    return [(512 * j, 512 if j < k - 1 else n - 512 * j) for j in range(k)]


def fwd_kernel(
    x_ref, wg_ref, wu_ref, wd_ref,
    WG, WU, WD, G, U, H, A, h1_ref,
    sg, su, sd, a_v, x_v, hid_v, bg, bu, wd_v, st_g, st_u,
    io, ld, out_s, loc, own_s, own_r, rx_s, rx_r, dd_s, dd_r, pp_s, pp_r, pd_s, pd_r,
):
    tokens, d = x_v.shape
    steps = tokens // BM
    rep, me = lax.axis_index("rep"), lax.axis_index("dp")
    chips = 4
    xx, c = me // 2, lax.rem(me, 2)
    right = lax.rem(xx + 1, chips) * 2 + c
    left = lax.rem(xx + chips - 1, chips) * 2 + c
    opp = lax.rem(xx + 2, chips) * 2 + c
    core = xx * 2 + (1 - c)
    p = lax.rem(rep, 2)
    pair = rep + 1 - 2 * p
    to_right, to_left, to_core = {"dp": right}, {"dp": left}, {"dp": core}
    to_pair = {"rep": pair}
    others = [lax.rem(xx + k, chips) * 2 + (1 - c) for k in (chips - 1, 1, 2, 2)]
    mine = [left, right, opp, opp]

    shards = {"g": sg, "u": su, "d": sd}
    inputs = {"g": wg_ref, "u": wu_ref, "d": wd_ref}
    whole = {"g": WG, "u": WU, "d": WD}
    order = [("g", 0), ("u", 0), ("d", 0), ("g", 1), ("u", 1), ("d", 1)]
    number = {key: k for k, key in enumerate(order)}
    ring = [("g", 0, 0), ("u", 0, 0), ("g", 0, 1), ("u", 0, 1), ("d", 0, 0), ("d", 0, 1),
            ("g", 1, 0), ("u", 1, 0), ("g", 1, 1), ("u", 1, 1), ("d", 1, 0), ("d", 1, 1)]

    def extent(kind, pos):
        rows, cols = shards[kind].shape[1:]
        n, unit = (rows, 16) if kind == "d" else (cols, 128)
        w = thirds(n, unit)
        far = n - w[2]
        off = (p * far, w[0], (1 - p) * far)[pos]
        if pos != 1:
            off = pl.multiple_of(off, unit)
        return (off, w[pos], 0, cols) if kind == "d" else (0, rows, off, w[pos])

    def region(ref, kind, layer, pos, base, half=None):
        r0, rows, c0, cols = extent(kind, pos)
        if half is not None:
            first = (rows // 2 + 15) // 16 * 16
            r0, rows = (r0, first) if half == 0 else (r0 + first, rows - first)
        start = r0 + base
        if not isinstance(start, int):
            start = pl.multiple_of(start, 16)
        return ref.at[layer, pl.ds(start, rows), pl.ds(c0, cols)]

    def place(kind, layer, pos, shard, half=None):
        return region(whole[kind], kind, layer, pos, shard * shards[kind].shape[1], half)

    def remote(src, dst, ss, rs, to):
        return pltpu.make_async_remote_copy(src_ref=src, dst_ref=dst, send_sem=ss, recv_sem=rs, device_id=to, device_id_type=MESH)

    def got(dst, ss, rs):
        remote(dst, dst, ss, rs, to_core).wait_recv()

    HALF = (None, None, 0, 1)

    def send_ring(k, j):
        kind, layer, pos = ring[k]
        if j < 2:
            src = region(shards[kind], kind, layer, pos, 0)
            dst = place(kind, layer, pos, me)
            return remote(src, dst, rx_s.at[k, j], rx_r.at[k, j], (to_right, to_left)[j])
        shard = (left, right)[j - 2]
        at = place(kind, layer, pos, shard, j - 2)
        return remote(at, at, rx_s.at[k, j], rx_r.at[k, j], (to_right, to_left)[j - 2])

    def recv_ring(k, j):
        kind, layer, pos = ring[k]
        got(place(kind, layer, pos, mine[j], HALF[j]), rx_s.at[k, j], rx_r.at[k, j])

    def send_core(k, j):
        kind, layer, pos = ring[k]
        at = place(kind, layer, pos, mine[j], HALF[j])
        return remote(at, at, dd_s.at[k, j], dd_r.at[k, j], to_core)

    def recv_core(k, j):
        kind, layer, pos = ring[k]
        got(place(kind, layer, pos, others[j], HALF[j]), dd_s.at[k, j], dd_r.at[k, j])

    def send_pair(k, j):
        kind, layer, pos = ring[k]
        q = number[kind, layer]
        at = place(kind, layer, pos, mine[j], HALF[j])
        return remote(at, at, pp_s.at[q, j], pp_r.at[q, j], to_pair)

    def recv_pair(q, j):
        kind, layer = order[q]
        got(place(kind, layer, 2, mine[j], HALF[j]), pp_s.at[q, j], pp_r.at[q, j])

    def send_pair_core(q, j):
        kind, layer = order[q]
        at = place(kind, layer, 2, mine[j], HALF[j])
        return remote(at, at, pd_s.at[q, j], pd_r.at[q, j], to_core)

    def recv_pair_core(q, j):
        kind, layer = order[q]
        got(place(kind, layer, 2, others[j], HALF[j]), pd_s.at[q, j], pd_r.at[q, j])

    def slot_of(kind, layer, shard):
        rows = shards[kind].shape[1]
        return whole[kind].at[layer, pl.ds(pl.multiple_of(shard * rows, 16), rows), :]

    def send_own(q):
        kind, layer = order[q]
        return remote(shards[kind].at[layer], slot_of(kind, layer, me), own_s.at[q], own_r.at[q], to_core)

    def recv_own(q):
        kind, layer = order[q]
        got(slot_of(kind, layer, core), own_s.at[q], own_r.at[q])

    def keep_own(q):
        kind, layer = order[q]
        return pltpu.make_async_copy(shards[kind].at[layer], slot_of(kind, layer, me), loc.at[q])

    def I(k):
        for j in (0, 1):
            send_ring(k, j).start()

    def onward(k, j):
        send_core(k, j).start()
        if ring[k][2] == 0:
            send_pair(k, j).start()

    def Fw(k):
        for j in (0, 1):
            recv_ring(k, j)
            send_ring(k, 2 + j).start()
            onward(k, j)

    def Gw(k):
        for j in (2, 3):
            recv_ring(k, j)
            onward(k, j)

    def Hw(q):
        for j in range(4):
            recv_pair(q, j)
            send_pair_core(q, j).start()

    def whole_piece(kind, layer, pos):
        if pos == 2:
            for j in range(4):
                recv_pair_core(number[kind, layer], j)
        else:
            for j in range(4):
                recv_core(ring.index((kind, layer, pos)), j)

    first = [pltpu.make_async_copy(inputs[kind], shards[kind], io.at[n]) for n, kind in enumerate("gud")]
    for copy in first:
        copy.start()
    load_x = pltpu.make_async_copy(x_ref, x_v, io.at[3])
    load_x.start()
    barrier = pltpu.get_barrier_semaphore()
    for to in (to_right, to_left, to_core, to_pair):
        pl.semaphore_signal(barrier, inc=1, device_id=to, device_id_type=MESH)
    pl.semaphore_wait(barrier, 4)
    for copy in first:
        copy.wait()
    I(0)
    I(1)
    for q in (0, 1):
        send_own(q).start()
        keep_own(q).start()
    load_x.wait()

    @pl.loop(0, steps)
    def _(m):
        rows = pl.ds(pl.multiple_of(m * BM, BM), BM)
        a_v[rows, :] = normed(x_v[rows, :].astype(F32))

    keep_a = [pltpu.make_async_copy(a_v, A.at[layer], io.at[4 + layer]) for layer in range(2)]
    keep_a[0].start()
    Fw(0)
    I(2)
    Fw(1)
    Gw(0)
    I(3)
    Gw(1)
    for q in range(2, 6):
        send_own(q).start()
        keep_own(q).start()
    for q in (0, 1):
        keep_own(q).wait()
        recv_own(q)

    widths = thirds(wg_ref.shape[2], 128)
    starts = (0, widths[0], widths[0] + widths[1])

    def load_weights(layer, pos):
        _, _, c0, cols = extent("g", pos)
        slot = pos % 2
        return [
            pltpu.make_async_copy(w.at[layer, :, pl.ds(c0, cols)], b.at[slot, :, pl.ds(0, cols)], ld.at[slot, n])
            for n, (w, b) in enumerate(((WG, bg), (WU, bu)))
        ]

    def store_out(layer, pos, m):
        _, _, c0, cols = extent("g", pos)
        slot = lax.rem(m, 2)
        rows = pl.ds(pl.multiple_of(m * BM, BM), BM)
        return [
            pltpu.make_async_copy(st_g.at[slot, :, pl.ds(0, cols)], G.at[layer, rows, pl.ds(c0, cols)], out_s.at[slot, 0]),
            pltpu.make_async_copy(st_u.at[slot, :, pl.ds(0, cols)], U.at[layer, rows, pl.ds(c0, cols)], out_s.at[slot, 1]),
            pltpu.make_async_copy(hid_v.at[rows, pl.ds(starts[pos], cols)], H.at[layer, rows, pl.ds(c0, cols)], out_s.at[slot, 2]),
        ]

    def gate_up(layer, pos, acts):
        cols = widths[pos]
        slot = pos % 2
        for copy in load_weights(layer, pos):
            copy.wait()

        @pl.loop(0, steps)
        def _(m):
            for at, todo in acts.items():

                @pl.when(m == at)
                def _():
                    for act in todo:
                        act()

            rows = pl.ds(pl.multiple_of(m * BM, BM), BM)
            back = lax.rem(m, 2)

            @pl.when(m >= 2)
            def _():
                for copy in store_out(layer, pos, m - 2):
                    copy.wait()

            if pos:

                @pl.when(m < 2)
                def _():
                    for copy in store_out(layer, pos - 1, m + steps - 2):
                        copy.wait()

            a = a_v[rows, :]
            for c0, w in cuts(cols):
                gate = dot(a, bg[slot, :, c0 : c0 + w])
                up = dot(a, bu[slot, :, c0 : c0 + w])
                st_g[back, :, c0 : c0 + w] = gate
                st_u[back, :, c0 : c0 + w] = up
                hid_v[rows, starts[pos] + c0 : starts[pos] + c0 + w] = (gate * jax.nn.sigmoid(gate) * up).astype(BF16)
            for copy in store_out(layer, pos, m):
                copy.start()

        if pos == 2:
            for m in (steps - 2, steps - 1):
                for copy in store_out(layer, pos, m):
                    copy.wait()

    def ready(layer, pos):
        def act():
            for kind in "gu":
                whole_piece(kind, layer, pos)
            for copy in load_weights(layer, pos):
                copy.start()

        return act

    def then(*acts):
        for act in acts:
            act()

    P_ = functools.partial
    ready(0, 0)()
    gate_up(0, 0, {3: [P_(Fw, 2), P_(I, 4)], 6: [P_(Gw, 2)]})
    then(P_(Fw, 3), P_(I, 5), P_(Gw, 3), ready(0, 1))
    gate_up(0, 1, {0: [P_(Hw, 0)], 3: [P_(Fw, 4), P_(I, 6), P_(Hw, 1)], 6: [P_(Gw, 4)], 7: [ready(0, 2)]})
    gate_up(0, 2, {1: [P_(Fw, 5), P_(I, 7)], 4: [P_(Gw, 5)]})

    load_wd = []
    for n in range(3):
        _, _, c0, cols = extent("g", n)
        load_wd.append(pltpu.make_async_copy(WD.at[0, pl.ds(c0, cols), :], wd_v.at[pl.ds(starts[n], cols), :], io.at[6 + n]))
    Hw(2)
    keep_own(2).wait()
    recv_own(2)
    for pos in (0, 1, 2):
        whole_piece("d", 0, pos)
    for copy in load_wd:
        copy.start()
    then(P_(Fw, 6), P_(I, 8))
    keep_a[0].wait()
    for copy in load_wd:
        copy.wait()

    def own_1():
        for q in (3, 4):
            keep_own(q).wait()
            recv_own(q)

    acts = {1: [P_(Gw, 6)], 4: [P_(Fw, 7), P_(I, 9)], 6: [P_(Gw, 7)], 7: [own_1, ready(1, 0)]}

    @pl.loop(0, steps)
    def _(m):
        for at, todo in acts.items():

            @pl.when(m == at)
            def _():
                for act in todo:
                    act()

        rows = pl.ds(pl.multiple_of(m * BM, BM), BM)
        h = x_v[rows, :] + dot(hid_v[rows, :], wd_v[...]).astype(BF16)
        x_v[rows, :] = h
        a_v[rows, :] = normed(h.astype(F32))

    keep_h = pltpu.make_async_copy(x_v, h1_ref, io.at[9])
    keep_h.start()
    keep_a[1].start()
    gate_up(1, 0, {1: [P_(Fw, 8), P_(I, 10)], 3: [P_(Gw, 8), P_(Hw, 3)]})
    then(P_(Fw, 9), P_(I, 11), P_(Gw, 9), ready(1, 1))
    gate_up(1, 1, {3: [P_(Fw, 10)], 5: [P_(Gw, 10), P_(Hw, 4)], 7: [ready(1, 2)]})
    gate_up(1, 2, {2: [P_(Fw, 11)], 4: [P_(Gw, 11)]})
    Hw(5)
    keep_own(5).wait()
    recv_own(5)
    for pos in (0, 1, 2):
        whole_piece("d", 1, pos)
    keep_h.wait()
    keep_a[1].wait()
    for k in range(len(ring)):
        for j in range(4):
            send_ring(k, j).wait_send()
            send_core(k, j).wait_send()
            if ring[k][2] == 0:
                send_pair(k, j).wait_send()
    for q in range(len(order)):
        send_own(q).wait_send()
        for j in range(4):
            send_pair_core(q, j).wait_send()


def forward(x, wg, wu, wd):
    tokens, d = x.shape
    layers, _, ff = wg.shape
    dma = lambda *s: pltpu.SemaphoreType.DMA(s)
    big = max(thirds(ff, 128))
    like = lambda s, t=BF16: jax.ShapeDtypeStruct(s, t)
    return pl.pallas_call(
        fwd_kernel,
        name="forward",
        in_specs=[ANY] * 4,
        out_specs=[ANY] * 8,
        out_shape=[
            like((layers, d, ff)), like((layers, d, ff)), like((layers, ff, d)),
            like((layers, tokens, ff), F32), like((layers, tokens, ff), F32), like((layers, tokens, ff)),
            like((layers, tokens, d)), like((tokens, d)),
        ],
        scratch_shapes=[
            pltpu.VMEM(wg.shape, BF16), pltpu.VMEM(wu.shape, BF16), pltpu.VMEM(wd.shape, BF16),
            pltpu.VMEM((tokens, d), BF16), pltpu.VMEM((tokens, d), BF16), pltpu.VMEM((tokens, ff), BF16),
            pltpu.VMEM((2, d, big), BF16), pltpu.VMEM((2, d, big), BF16), pltpu.VMEM((ff, d), BF16),
            pltpu.VMEM((2, BM, big), F32), pltpu.VMEM((2, BM, big), F32),
            dma(10), dma(2, 2), dma(2, 3), dma(6), dma(6), dma(6), dma(12, 4), dma(12, 4), dma(12, 4), dma(12, 4),
            dma(6, 4), dma(6, 4), dma(6, 4), dma(6, 4),
        ],
        compiler_params=pltpu.CompilerParams(collective_id=0, has_side_effects=True, vmem_limit_bytes=64 * MB - 64 * 1024),
        cost_estimate=pl.CostEstimate(flops=10 * tokens * d * ff, bytes_accessed=200 * MB, transcendentals=0),
    )(x, wg, wu, wd)


def call(body, name, grid, in_specs, out_specs, out_shape, mats):
    return pl.pallas_call(
        body,
        name=name,
        grid=grid,
        in_specs=in_specs,
        out_specs=out_specs,
        out_shape=out_shape,
        compiler_params=pltpu.CompilerParams(vmem_limit_bytes=60 * MB),
        cost_estimate=pl.CostEstimate(flops=int(mats * 2 * 2048 * 1024 * 3200), bytes_accessed=20 * MB, transcendentals=0),
    )


def by_weight(a, b, layer, bm, bn, name):
    tokens, m = a.shape[-2:]
    n = b.shape[-1]

    def body(a_ref, b_ref, o_ref):
        o_ref[...] = dot(a_ref[...].reshape(tokens, bm), b_ref[...], 0, 0).astype(BF16)

    spec = pl.BlockSpec((None, tokens, bm), lambda j, i: (layer, 0, i)) if a.ndim == 3 else pl.BlockSpec((tokens, bm), lambda j, i: (0, i))
    return call(
        body, name, (n // bn, m // bm), [spec, pl.BlockSpec((tokens, bn), lambda j, i: (0, j))],
        pl.BlockSpec((bm, bn), lambda j, i: (i, j)), jax.ShapeDtypeStruct((m, n), BF16), 1,
    )(a, b)


def by_gates(by_h, WD, G, U, layer, name):
    tokens, d = by_h.shape
    ff = WD.shape[1]
    bm, bn = 512, 640

    def body(by_ref, w_ref, g_ref, u_ref, dg_ref, du_ref):
        by = by_ref[...]
        for c0, w in cuts(bn):
            dh = dot(by, w_ref[c0 : c0 + w, :], 1, 1).astype(BF16).astype(F32)
            gate, up = g_ref[:, c0 : c0 + w], u_ref[:, c0 : c0 + w]
            sig = jax.nn.sigmoid(gate)
            silu = gate * sig
            du_ref[:, c0 : c0 + w] = (dh * silu).astype(BF16)
            dg_ref[:, c0 : c0 + w] = (dh * up * (sig + silu * (1 - sig))).astype(BF16)

    wide = pl.BlockSpec((None, bm, bn), lambda j, i: (layer, i, j))
    out = pl.BlockSpec((bm, bn), lambda j, i: (i, j))
    return call(
        body, name, (ff // bn, tokens // bm),
        [pl.BlockSpec((bm, d), lambda j, i: (i, 0)), pl.BlockSpec((None, bn, d), lambda j, i: (layer, j, 0)), wide, wide],
        [out, out], [jax.ShapeDtypeStruct((tokens, ff), BF16)] * 2, 1,
    )(by_h, WD, G, U)


def by_states(dg, du, WG, WU, h, by_h, layer, name):
    tokens, ff = dg.shape
    d = h.shape[1]
    bm = 256

    def body(dg_ref, du_ref, wg_ref, wu_ref, h_ref, by_ref, o_ref):
        da = dot(dg_ref[...], wg_ref[...], 1, 1).astype(BF16).astype(F32) + dot(du_ref[...], wu_ref[...], 1, 1).astype(BF16).astype(F32)
        da = da.astype(BF16).astype(F32)
        wide = h_ref[...].astype(F32)
        scale = lax.rsqrt(jnp.mean(wide * wide, -1, keepdims=True) + 1e-6)
        along = jnp.mean(da * wide, -1, keepdims=True)
        by = da * scale - wide * (scale * scale * scale * along)
        o_ref[...] = by_ref[...] + by.astype(BF16)

    rows = pl.BlockSpec((bm, ff), lambda i: (i, 0))
    full = pl.BlockSpec((None, d, ff), lambda i: (layer, 0, 0))
    out = pl.BlockSpec((bm, d), lambda i: (i, 0))
    return call(body, name, (tokens // bm,), [rows, rows, full, full, out, out], out, jax.ShapeDtypeStruct((tokens, d), BF16), 2)(
        dg, du, WG, WU, h, by_h
    )


def adamw(w, m, v, g):
    m = 0.9 * m + 0.1 * g
    v = 0.95 * v + 0.05 * g * g
    step = m * lax.rsqrt(v + 1e-8) + 0.1 * w
    return (w - 0.02 * step).astype(jnp.bfloat16), m, v


def solution(mesh):
    def step(x, dy, *arrays):
        weights, m, v = (arrays[i : i + 3] for i in (0, 3, 6))
        x, dy = x[0], dy[0]
        WG, WU, WD, G, U, H, A, h1 = forward(x, *weights)
        scatter = lambda g: lax.psum_scatter(g, "dp", scatter_dimension=0, tiled=True)
        d1 = scatter(by_weight(H, dy, 1, 640, 1024, "dw_down1"))
        dg, du = by_gates(dy, WD, G, U, 1, "gates1")
        g1 = scatter(by_weight(A, dg, 1, 1024, 640, "dw_gate1"))
        u1 = scatter(by_weight(A, du, 1, 1024, 640, "dw_up1"))
        by_h = by_states(dg, du, WG, WU, h1, dy, 1, "states1")
        d0 = scatter(by_weight(H, by_h, 0, 640, 1024, "dw_down0"))
        dg, du = by_gates(by_h, WD, G, U, 0, "gates0")
        g0 = scatter(by_weight(A, dg, 0, 1024, 640, "dw_gate0"))
        u0 = scatter(by_weight(A, du, 0, 1024, 640, "dw_up0"))
        gradients = [jnp.stack(pair).astype(F32) for pair in ((g0, g1), (u0, u1), (d0, d1))]
        new = [adamw(w.astype(F32), m, v, g) for w, m, v, g in zip(weights, m, v, gradients, strict=True)]
        return tuple(one[which] for which in range(3) for one in new)

    states, cut = P(("rep", "dp"), None, None), P(None, "dp", None)
    return jax.shard_map(
        step,
        mesh=mesh,
        in_specs=(states, states) + (cut,) * 9,
        out_specs=(P("rep", "dp", None),) * 9,
        check_vma=False,
    )
```

```python
import re

import jax
import jax.numpy as jnp
from jax import lax
from jax.experimental import pallas as pl
from jax.experimental.pallas import tpu as pltpu
from jax.sharding import PartitionSpec as P

MESH = pl.DeviceIdType.MESH
F32, BF16 = jnp.float32, jnp.bfloat16
ANY = pl.BlockSpec(memory_space=pl.ANY)
BM = 512
MB = 2**20


def dot(a, b, ca=1, cb=0):
    return lax.dot_general(a, b, (((ca,), (cb,)), ((), ())), preferred_element_type=F32)


def normed(wide):
    scale = lax.rsqrt(jnp.mean(wide * wide, -1, keepdims=True) + 1e-6)
    return (wide * scale).astype(BF16)


def by_gate(gate, up, dh):
    sig = 0.5 * jnp.tanh(0.5 * gate) + 0.5
    silu = gate * sig
    return silu, (dh * up * (sig + silu * (1 - sig))).astype(BF16), (dh * silu).astype(BF16)


def plan(text):
    steps = {}
    for step, act, number in re.findall(r"(\d*)([A-Za-z])(\d+)", text):
        steps.setdefault(int(step or "0"), []).append((act, int(number)))
    return steps


def thirds(n, unit):
    tiles = n // unit
    side = tiles // 3
    return side * unit, (tiles - 2 * side) * unit, side * unit


def cuts(n):
    k = max(1, n // 512)
    return [(512 * j, 512 if j < k - 1 else n - 512 * j) for j in range(k)]


def fwd_kernel(
    x_ref, dy_ref, wg_ref, wu_ref, wd_ref,
    WG, WU, WD, G, U, H, A, h1_ref, DGU,
    sg, su, sd, a_v, x_v, hid_v, bg, bu, wd_v, st_g, st_u, st_d,
    io, ld, out_s, loc, own_s, own_r, rx_s, rx_r, dd_s, dd_r, pp_s, pp_r, pd_s, pd_r,
):
    tokens, d = x_v.shape
    steps = tokens // BM
    rep, me = lax.axis_index("rep"), lax.axis_index("dp")
    chips = 4
    xx, c = me // 2, lax.rem(me, 2)
    right = lax.rem(xx + 1, chips) * 2 + c
    left = lax.rem(xx + chips - 1, chips) * 2 + c
    opp = lax.rem(xx + 2, chips) * 2 + c
    core = xx * 2 + (1 - c)
    p = lax.rem(rep, 2)
    pair = rep + 1 - 2 * p
    to_right, to_left, to_core = {"dp": right}, {"dp": left}, {"dp": core}
    to_pair = {"rep": pair}
    others = [lax.rem(xx + k, chips) * 2 + (1 - c) for k in (chips - 1, 1, 2, 2)]
    mine = [left, right, opp, opp]

    shards = {"g": sg, "u": su, "d": sd}
    inputs = {"g": wg_ref, "u": wu_ref, "d": wd_ref}
    whole = {"g": WG, "u": WU, "d": WD}
    order = [(kind, 0) for kind in "gud"] + [(kind, 1) for kind in "dgu"]
    number = {key: k for k, key in enumerate(order)}
    ring = [(name[0], int(name[1]), int(name[2])) for name in "g00 u00 g01 u01".split() + "d00 d01 d10 d11".split() + "g10 u10 g11 u11".split()]

    def extent(kind, pos):
        rows, cols = shards[kind].shape[1:]
        n, unit = (rows, 16) if kind == "d" else (cols, 128)
        w = thirds(n, unit)
        far = n - w[2]
        off = (p * far, w[0], (1 - p) * far)[pos]
        if pos != 1:
            off = pl.multiple_of(off, unit)
        return (off, w[pos], 0, cols) if kind == "d" else (0, rows, off, w[pos])

    def region(ref, kind, layer, pos, base, half=None):
        r0, rows, c0, cols = extent(kind, pos)
        if half is not None:
            first = (rows // 2 + 15) // 16 * 16
            r0, rows = (r0, first) if half == 0 else (r0 + first, rows - first)
        start = r0 + base
        if not isinstance(start, int):
            start = pl.multiple_of(start, 16)
        return ref.at[layer, pl.ds(start, rows), pl.ds(c0, cols)]

    def place(kind, layer, pos, shard, half=None):
        return region(whole[kind], kind, layer, pos, shard * shards[kind].shape[1], half)

    def remote(src, dst, ss, rs, to):
        return pltpu.make_async_remote_copy(src_ref=src, dst_ref=dst, send_sem=ss, recv_sem=rs, device_id=to, device_id_type=MESH)

    def got(dst, ss, rs):
        remote(dst, dst, ss, rs, to_core).wait_recv()

    HALF = (None, None, 0, 1)

    def send_ring(k, j):
        kind, layer, pos = ring[k]
        if j < 2:
            src = region(shards[kind], kind, layer, pos, 0)
            dst = place(kind, layer, pos, me)
            return remote(src, dst, rx_s.at[k, j], rx_r.at[k, j], (to_right, to_left)[j])
        shard = (left, right)[j - 2]
        at = place(kind, layer, pos, shard, j - 2)
        return remote(at, at, rx_s.at[k, j], rx_r.at[k, j], (to_right, to_left)[j - 2])

    def recv_ring(k, j):
        kind, layer, pos = ring[k]
        got(place(kind, layer, pos, mine[j], HALF[j]), rx_s.at[k, j], rx_r.at[k, j])

    def send_core(k, j):
        kind, layer, pos = ring[k]
        at = place(kind, layer, pos, mine[j], HALF[j])
        return remote(at, at, dd_s.at[k, j], dd_r.at[k, j], to_core)

    def recv_core(k, j):
        kind, layer, pos = ring[k]
        got(place(kind, layer, pos, others[j], HALF[j]), dd_s.at[k, j], dd_r.at[k, j])

    def send_pair(k, j):
        kind, layer, pos = ring[k]
        q = number[kind, layer]
        at = place(kind, layer, pos, mine[j], HALF[j])
        return remote(at, at, pp_s.at[q, j], pp_r.at[q, j], to_pair)

    def recv_pair(q, j):
        kind, layer = order[q]
        got(place(kind, layer, 2, mine[j], HALF[j]), pp_s.at[q, j], pp_r.at[q, j])

    def send_pair_core(q, j):
        kind, layer = order[q]
        at = place(kind, layer, 2, mine[j], HALF[j])
        return remote(at, at, pd_s.at[q, j], pd_r.at[q, j], to_core)

    def recv_pair_core(q, j):
        kind, layer = order[q]
        got(place(kind, layer, 2, others[j], HALF[j]), pd_s.at[q, j], pd_r.at[q, j])

    def slot_of(kind, layer, shard):
        rows = shards[kind].shape[1]
        return whole[kind].at[layer, pl.ds(pl.multiple_of(shard * rows, 16), rows), :]

    def send_own(q):
        kind, layer = order[q]
        return remote(shards[kind].at[layer], slot_of(kind, layer, me), own_s.at[q], own_r.at[q], to_core)

    def recv_own(q):
        kind, layer = order[q]
        got(slot_of(kind, layer, core), own_s.at[q], own_r.at[q])

    def keep_own(q):
        kind, layer = order[q]
        return pltpu.make_async_copy(shards[kind].at[layer], slot_of(kind, layer, me), loc.at[q])

    def I(k):
        for j in range(2):
            send_ring(k, j).start()

    def onward(k, j):
        send_core(k, j).start()
        if ring[k][2] == 0:
            send_pair(k, j).start()

    def Fw(k):
        for j in range(2):
            recv_ring(k, j)
            send_ring(k, 2 + j).start()
            onward(k, j)

    def Gw(k):
        for j in (2, 3):
            recv_ring(k, j)
            onward(k, j)

    def Hw(q):
        for j in range(4):
            recv_pair(q, j)
            send_pair_core(q, j).start()

    def whole_piece(kind, layer, pos):
        if pos == 2:
            for j in range(4):
                recv_pair_core(number[kind, layer], j)
        else:
            for j in range(4):
                recv_core(ring.index((kind, layer, pos)), j)

    def head():
        for act, n in plan("F0,I2,F1,I3,G0,F2,I4,G1")[0]:
            {"I": I, "F": Fw, "G": Gw}[act](n)

    first = [pltpu.make_async_copy(inputs[kind], shards[kind], io.at[n]) for n, kind in enumerate("gud")]
    for copy in first:
        copy.start()
    load_x = pltpu.make_async_copy(x_ref, x_v, io.at[3])
    load_x.start()
    barrier = pltpu.get_barrier_semaphore()
    for to in (to_right, to_left, to_core, to_pair):
        pl.semaphore_signal(barrier, inc=1, device_id=to, device_id_type=MESH)
    pl.semaphore_wait(barrier, 4)
    for copy in first:
        copy.wait()
    I(0)
    I(1)
    for q in range(2):
        send_own(q).start()
        keep_own(q).start()
    load_x.wait()

    @pl.loop(0, steps)
    def _(m):
        rows = pl.ds(pl.multiple_of(m * BM, BM), BM)
        a_v[rows, :] = normed(x_v[rows, :].astype(F32))

    keep_a = [pltpu.make_async_copy(a_v, A.at[layer], io.at[4 + layer]) for layer in range(2)]
    keep_a[0].start()
    head()
    for q in range(2, 6):
        send_own(q).start()
        keep_own(q).start()
    for q in range(2):
        keep_own(q).wait()
        recv_own(q)

    widths = thirds(wg_ref.shape[2], 128)
    starts = (0, widths[0], widths[0] + widths[1])

    def load_weights(layer, pos):
        _, _, c0, cols = extent("g", pos)
        slot = pos % 2
        return [
            pltpu.make_async_copy(w.at[layer, :, pl.ds(c0, cols)], b.at[slot, :, pl.ds(0, cols)], ld.at[slot, n])
            for n, (w, b) in enumerate(((WG, bg), (WU, bu)))
        ]

    def store_out(layer, pos, m):
        _, _, c0, cols = extent("g", pos)
        slot = lax.rem(m, 2)
        rows = pl.ds(pl.multiple_of(m * BM, BM), BM)
        if layer:
            copies = [
                pltpu.make_async_copy(st_d.at[slot, n, :, pl.ds(0, cols)], DGU.at[n, rows, pl.ds(c0, cols)], out_s.at[slot, n])
                for n in range(2)
            ]
        else:
            copies = [
                pltpu.make_async_copy(st.at[slot, :, pl.ds(0, cols)], out.at[rows, pl.ds(c0, cols)], out_s.at[slot, n])
                for n, (st, out) in enumerate(((st_g, G), (st_u, U)))
            ]
        return copies + [
            pltpu.make_async_copy(hid_v.at[rows, pl.ds(starts[pos], cols)], H.at[layer, rows, pl.ds(c0, cols)], out_s.at[slot, 2]),
        ]

    def gate_up(layer, pos, acts):
        cols = widths[pos]
        slot = pos % 2
        for copy in load_weights(layer, pos):
            copy.wait()

        @pl.loop(0, steps)
        def _(m):
            at_step(m, acts)
            rows = pl.ds(pl.multiple_of(m * BM, BM), BM)
            back = lax.rem(m, 2)

            @pl.when(m >= 2)
            def _():
                for copy in store_out(layer, pos, m - 2):
                    copy.wait()

            if pos:

                @pl.when(m < 2)
                def _():
                    for copy in store_out(layer, pos - 1, m + steps - 2):
                        copy.wait()

            a = a_v[rows, :]
            for c0, w in cuts(cols):
                gate = dot(a, bg[slot, :, c0 : c0 + w])
                up = dot(a, bu[slot, :, c0 : c0 + w])
                at = starts[pos] + c0
                if layer:
                    dh = dot(x_v[rows, :], wd_v[at : at + w, :], 1, 1).astype(BF16).astype(F32)
                    silu, dg, du = by_gate(gate, up, dh)
                    st_d[back, 0, :, c0 : c0 + w] = dg
                    st_d[back, 1, :, c0 : c0 + w] = du
                else:
                    st_g[back, :, c0 : c0 + w] = gate
                    st_u[back, :, c0 : c0 + w] = up
                    silu = gate * (0.5 * jnp.tanh(0.5 * gate) + 0.5)
                hid_v[rows, at : at + w] = (silu * up).astype(BF16)
            for copy in store_out(layer, pos, m):
                copy.start()

        if pos == 2:
            for m in (steps - 2, steps - 1):
                for copy in store_out(layer, pos, m):
                    copy.wait()

    def ready(layer, pos):
        def act():
            for kind in "gu":
                whole_piece(kind, layer, pos)
            for copy in load_weights(layer, pos):
                copy.start()

        return act

    def then(acts):
        for todo in plan(acts).values():
            for act, n in todo:
                moves[act](n)

    def R(n):
        ready(n // 3, n % 3)()

    def O(_):
        own_1()

    moves = {"I": I, "F": Fw, "G": Gw, "H": Hw, "R": R, "O": O}

    def at_step(m, acts):
        for when, todo in plan(acts).items():

            @pl.when(m == when)
            def _():
                for act, n in todo:
                    moves[act](n)

    def load_down(layer):
        copies = []
        for n in range(3):
            _, _, c0, cols = extent("g", n)
            copies.append(pltpu.make_async_copy(WD.at[layer, pl.ds(c0, cols), :], wd_v.at[pl.ds(starts[n], cols), :], io.at[6 + n]))
        return copies

    def start_down(layer):
        q = number["d", layer]
        keep_own(q).wait()
        recv_own(q)
        for pos in range(3):
            whole_piece("d", layer, pos)
        for copy in load_down(layer):
            copy.start()

    def own_1():
        for q in (4, 5):
            keep_own(q).wait()
            recv_own(q)

    then("R0")
    gate_up(0, 0, "2F3,2I5,3G2")
    then("F4,I6,G3,R1")
    gate_up(0, 1, "1H0,1F5,1I7,3G4,3H1,3R2")
    gate_up(0, 2, "0F6,0I8,1G5,2H2,3F7,3I9")
    start_down(0)
    keep_a[0].wait()
    for copy in load_down(0):
        copy.wait()
    half = BM // 2

    @pl.loop(0, 2 * steps)
    def _(m):
        at_step(m, "0G6,3F8,5G7,7H3,7O0")
        rows = pl.ds(pl.multiple_of(m * half, half), half)
        h = x_v[rows, :] + dot(hid_v[rows, :], wd_v[...]).astype(BF16)
        x_v[rows, :] = h
        a_v[rows, :] = normed(h.astype(F32))

    keep_h = pltpu.make_async_copy(x_v, h1_ref, io.at[9])
    keep_h.start()
    keep_a[1].start()
    start_down(1)
    then("F9,I10,I11,G8")
    keep_h.wait()
    load_dy = pltpu.make_async_copy(dy_ref, x_v, io.at[3])
    load_dy.start()
    then("G9,R3")
    for copy in load_down(1):
        copy.wait()
    load_dy.wait()
    gate_up(1, 0, "2F10,3F11,3G10")
    then("G11,R4")
    gate_up(1, 1, "1H4,1H5,3R5")
    gate_up(1, 2, "")
    keep_a[1].wait()
    for k in range(len(ring)):
        for j in range(4):
            send_ring(k, j).wait_send()
            send_core(k, j).wait_send()
            if ring[k][2] == 0:
                send_pair(k, j).wait_send()
    for q in range(len(order)):
        send_own(q).wait_send()
        for j in range(4):
            send_pair_core(q, j).wait_send()


def forward(x, dy, wg, wu, wd):
    tokens, d = x.shape
    layers, _, ff = wg.shape
    dma = lambda *s: pltpu.SemaphoreType.DMA(s)
    big = max(thirds(ff, 128))
    like = lambda s, t=BF16: jax.ShapeDtypeStruct(s, t)
    return pl.pallas_call(
        fwd_kernel,
        name="forward",
        in_specs=[ANY] * 5,
        out_specs=[ANY] * 9,
        out_shape=[
            like((layers, d, ff)), like((layers, d, ff)), like((layers, ff, d)),
            like((tokens, ff), F32), like((tokens, ff), F32), like((layers, tokens, ff)),
            like((layers, tokens, d)), like((tokens, d)), like((2, tokens, ff)),
        ],
        scratch_shapes=[
            pltpu.VMEM(wg.shape, BF16), pltpu.VMEM(wu.shape, BF16), pltpu.VMEM(wd.shape, BF16),
            pltpu.VMEM((tokens, d), BF16), pltpu.VMEM((tokens, d), BF16), pltpu.VMEM((tokens, ff), BF16),
            pltpu.VMEM((2, d, big), BF16), pltpu.VMEM((2, d, big), BF16), pltpu.VMEM((ff, d), BF16),
            pltpu.VMEM((2, BM, big), F32), pltpu.VMEM((2, BM, big), F32), pltpu.VMEM((2, 2, BM, big), BF16),
            dma(10), dma(2, 2), dma(2, 3), *[dma(6)] * 3, *[dma(12, 4)] * 4, *[dma(6, 4)] * 4,
        ],
        compiler_params=pltpu.CompilerParams(collective_id=0, has_side_effects=True, vmem_limit_bytes=64 * MB - 64 * 1024),
        cost_estimate=pl.CostEstimate(flops=10 * tokens * d * ff, bytes_accessed=200 * MB, transcendentals=0),
    )(x, dy, wg, wu, wd)


def adamw(w, m, v, g):
    m = 0.9 * m + 0.1 * g
    v = 0.95 * v + 0.05 * g * g
    step = m * lax.rsqrt(v + 1e-8) + 0.1 * w
    return (w - 0.02 * step).astype(jnp.bfloat16), m, v


def bwd_kernel(
    dy_ref, h_ref, A, H, G, U, WG, WU, WD, DGU,
    gd, gg, gu, DGU0, Dd, Dgu, Pd, Pg, Pu, Hd, Hg, Hu, Ld, Lg, Lu, Rd, Rg, Ru,
    v0, v1, wd_v, wg_v, wu_v, big_d, big_g,
    io, ld, ost, ds, dr, hs, hr, fs, fr,
):
    tokens, d = v0.shape
    ff = wd_v.shape[0]
    me = lax.axis_index("dp")
    chips = 4
    xx, c = me // 2, lax.rem(me, 2)
    ahead = [lax.rem(xx + k, chips) for k in range(chips)]
    to_right, to_left = {"dp": ahead[1] * 2 + c}, {"dp": ahead[3] * 2 + c}
    to_core = {"dp": xx * 2 + (1 - c)}

    others = {"d": Pd, "g": Pg, "u": Pu}
    halves = {"d": Hd, "g": Hg, "u": Hu}
    lefts = {"d": Ld, "g": Lg, "u": Lu}
    rights = {"d": Rd, "g": Rg, "u": Ru}
    outs = {"d": gd, "g": gg, "u": gu}
    split = ff // 640 // 2 * 640
    rows_d = gd.shape[1]
    tasks = [("d", 1, 0, rows_d), ("g", 1, 0, ff), ("u", 1, 0, ff), ("d", 0, 0, rows_d)]
    tasks += [(kind, 0, r0, n) for kind in "gu" for r0, n in ((0, split), (split, ff - split))]
    before = []
    for k, (kind, *_) in enumerate(tasks):
        same = [q for q in range(k) if (tasks[q][0] == "d") == (kind == "d")]
        before.append(same[-1] if same else None)

    def remote(src, dst, ss, rs, to):
        return pltpu.make_async_remote_copy(src_ref=src, dst_ref=dst, send_sem=ss, recv_sem=rs, device_id=to, device_id_type=MESH)

    def own(k, chip, core):
        kind, layer, r0, n = tasks[k]
        shard = chip * 2 + core
        if kind == "d":
            return Dd.at[layer, pl.ds(pl.multiple_of(shard * rows_d, 16), n), :]
        return Dgu.at[layer, "gu".index(kind), shard, pl.ds(r0, n), :]

    def other(k, chip):
        kind, layer, r0, n = tasks[k]
        return others[kind].at[layer, chip, pl.ds(r0, n), :]

    def at(refs, k, half=None):
        kind, layer, r0, n = tasks[k]
        a, b = cut(n, half)
        return refs[kind].at[layer, pl.ds(r0 + a, b), :]

    def cut(n, half):
        if half is None:
            return 0, n
        first = (n // 2 + 15) // 16 * 16
        return (0, first) if half == 0 else (first, n - first)

    def buf(k, which, half=None):
        kind, _, _, n = tasks[k]
        a, b = cut(n, half)
        return (big_d if kind == "d" else big_g).at[which, pl.ds(a, b), :]

    def load(k, src, which):
        return pltpu.make_async_copy(src, buf(k, which), ld.at[0 if tasks[k][0] == "d" else 1, which])

    def add(k, out, terms, half=None):
        ref = big_d if tasks[k][0] == "d" else big_g
        a, n = cut(tasks[k][3], half)
        step = 64 if tasks[k][0] == "d" else 320

        def some(rows):
            total = ref[terms[0], rows, :].astype(F32)
            for t in terms[1:]:
                total += ref[t, rows, :].astype(F32)
            ref[out, rows, :] = total.astype(BF16)

        @pl.loop(0, n // step)
        def _(i):
            some(pl.ds(pl.multiple_of(a + i * step, 16), step))

        if n % step:
            some(pl.ds(a + n // step * step, n % step))

    def to_other(k, chip):
        return remote(own(k, chip, 1 - c), other(k, chip), ds.at[k, chip], dr.at[k, chip], to_core)

    def send_half(k, half):
        return remote(buf(k, 8, half), at(halves, k, half), hs.at[k, half], hr.at[k, half], (to_right, to_left)[half])

    def send_full(k, side):
        return remote(buf(k, 5 + side), at((lefts, rights)[side], k), fs.at[k, side], fr.at[k, side], (to_right, to_left)[side])

    def A_(k):
        for chip in range(chips):
            to_other(k, chip).start()

    def loads(k, what):
        two = lambda chip: [load(k, own(k, ahead[chip], c), 0), load(k, other(k, ahead[chip]), 1)]
        if what == "B":
            return two(2)
        if what == "C":
            return two(1) + [load(k, own(k, ahead[3], c), 2), load(k, other(k, ahead[3]), 3), load(k, at(halves, k), 4)]
        return two(0) + [load(k, at(lefts, k), 2), load(k, at(rights, k), 3)]

    def B0(k):
        for chip in range(chips):
            to_other(k, chip).wait_recv()
        for copy in loads(k, "B"):
            copy.start()

    def B1(k):
        for copy in loads(k, "B"):
            copy.wait()
        if before[k] is not None:
            for half in range(2):
                send_half(before[k], half).wait_send()
        add(k, 8, (0, 1))
        for half in range(2):
            send_half(k, half).start()

    def C0(k):
        for half in range(2):
            send_half(k, half).wait_recv()
        for copy in loads(k, "C"):
            copy.start()

    def C1(k):
        for copy in loads(k, "C"):
            copy.wait()
        if before[k] is not None:
            for side in range(2):
                send_full(before[k], side).wait_send()
        add(k, 5, (0, 1, 4), 0)
        add(k, 5, (0, 1), 1)
        send_full(k, 0).start()
        add(k, 6, (2, 3), 0)
        add(k, 6, (2, 3, 4), 1)
        send_full(k, 1).start()

    def result(k):
        return pltpu.make_async_copy(buf(k, 7), at(outs, k), ost.at[0 if tasks[k][0] == "d" else 1])

    def D0(k):
        for side in range(2):
            send_full(k, side).wait_recv()
        for copy in loads(k, "D"):
            copy.start()

    def D1(k):
        for copy in loads(k, "D"):
            copy.wait()
        if before[k] is not None:
            result(before[k]).wait()
        add(k, 7, range(4))
        result(k).start()

    ACTS = {"A": A_, "b": B0, "B": B1, "c": C0, "C": C1, "d": D0, "D": D1}

    def perform(todo):
        for name, k in todo:
            ACTS[name](k)

    def run(acts):
        for todo in plan(acts).values():
            perform(todo)

    def acts_at(step, acts):
        for when, todo in plan(acts).items():

            @pl.when(step == when)
            def _():
                perform(todo)

    def pipe(body, grid, ins, outs_, acts):
        def inner(indices, *refs):
            acts_at(indices.local_index, acts)
            body(indices.index, *refs)

        pltpu.emit_pipeline(
            inner, grid=grid, in_specs=[s for s, _ in ins], out_specs=[s for s, _ in outs_], _explicit_indices=True
        )(*[r for _, r in ins], *[r for _, r in outs_])

    BF = 640
    tall = pl.BlockSpec((tokens, BF), lambda j: (0, j))

    def dw_down(layer, acts):
        def body(_, a_ref, o_ref):
            for c0, w in cuts(d):
                o_ref[:, c0 : c0 + w] = dot(a_ref[...], v0[:, c0 : c0 + w], 0, 0).astype(BF16)

        pipe(body, (ff // BF,), [(tall, H.at[layer])], [(pl.BlockSpec((BF, d), lambda j: (j, 0)), Dd.at[layer])], acts)

    def dw_up(src, layer, acts):
        n = ff // BF

        def body(_, a_ref, o_ref):
            for c0, w in cuts(d):
                part = dot(a_ref[...], v1[:, c0 : c0 + w], 0, 0).astype(BF16)
                for s in range(w // 128):
                    o_ref[c0 // 128 + s, :, :] = part[:, 128 * s : 128 * s + 128]

        a_spec = pl.BlockSpec((None, tokens, BF), lambda s: (s // n, 0, s % n))
        spec = pl.BlockSpec((None, d // 128, BF, 128), lambda s: (s // n, 0, s % n, 0))
        pipe(body, (2 * n,), [(a_spec, src)], [(spec, Dgu.at[layer])], acts)

    def gates(acts):
        bm = 512

        def body(indices, g_ref, u_ref, dg_ref):
            j, i = indices
            by = v0[pl.ds(pl.multiple_of(i * bm, bm), bm), :]
            for c0, w in ((0, 256), (256, 384)):
                wd = wd_v[pl.ds(pl.multiple_of(j * BF + c0, 128), w), :]
                dh = dot(by, wd, 1, 1).astype(BF16).astype(F32)
                _, dg, du = by_gate(g_ref[:, c0 : c0 + w], u_ref[:, c0 : c0 + w], dh)
                dg_ref[0, :, c0 : c0 + w] = dg
                dg_ref[1, :, c0 : c0 + w] = du

        spec = pl.BlockSpec((bm, BF), lambda j, i: (i, j), pipeline_mode=pl.Buffered(3))
        out = pl.BlockSpec((2, bm, BF), lambda j, i: (0, i, j))
        pipe(body, (ff // BF, tokens // bm), [(spec, G), (spec, U)], [(out, DGU0)], acts)

    def states(acts):
        bm = 256

        def body(indices, dgu_ref, hh_ref):
            rows = pl.ds(pl.multiple_of(indices[0] * bm, bm), bm)
            da = dot(dgu_ref[0], wg_v[...], 1, 1).astype(BF16).astype(F32) + dot(dgu_ref[1], wu_v[...], 1, 1).astype(BF16).astype(F32)
            da = da.astype(BF16).astype(F32)
            wide = hh_ref[...].astype(F32)
            scale = lax.rsqrt(jnp.mean(wide * wide, -1, keepdims=True) + 1e-6)
            along = jnp.mean(da * wide, -1, keepdims=True)
            by = da * scale - wide * (scale * scale * scale * along)
            v0[rows, :] = v0[rows, :] + by.astype(BF16)

        spec = pl.BlockSpec((2, bm, ff), lambda i: (0, i, 0))
        pipe(body, (tokens // bm,), [(spec, DGU), (pl.BlockSpec((bm, d), lambda i: (i, 0)), h_ref)], [], acts)

    barrier = pltpu.get_barrier_semaphore()
    for to in (to_right, to_left, to_core):
        pl.semaphore_signal(barrier, inc=1, device_id=to, device_id_type=MESH)
    into = lambda src, dst, n: pltpu.make_async_copy(src, dst, io.at[n])
    c_dy, c_a1 = into(dy_ref, v0, 0), into(A.at[1], v1, 1)
    c_wg, c_wu = into(WG.at[1], wg_v, 3), into(WU.at[1], wu_v, 4)
    c_a0, c_wd0 = into(A.at[0], v1, 5), into(WD.at[0], wd_v, 6)
    c_dy.start()
    c_a1.start()
    pl.semaphore_wait(barrier, 3)
    c_dy.wait()
    dw_down(1, "")
    run("A0")
    c_a1.wait()
    c_wg.start()
    c_wu.start()
    c_wd0.start()
    dw_up(DGU, 1, "2b0,3B0,7A1,7c0,8C0")
    run("A2,b1,B1")
    c_a0.start()
    c_wg.wait()
    c_wu.wait()
    states("2b2,3B2,4d0,5D0,6c1,7C1")
    dw_down(0, "0c2,1C2,4d1")
    run("A3,D1")
    c_wd0.wait()
    c_a0.wait()
    gates("5b3,6B3,9d2,10D2,15c3,16C3")
    dw_up(
        DGU0, 0,
        "4A4,4d3,5D3,6b4,7B4,7A5,9b5",
    )
    run("A6,A7,B5,c4,C4,b6,B6,c5,C5,b7,B7,d4,D4")
    run("c6,C6,c7,C7,d5,D5,d6,D6,d7,D7")
    for k in range(len(tasks)):
        for chip in range(chips):
            to_other(k, chip).wait_send()
        if k not in before:
            result(k).wait()
            for side in range(2):
                send_full(k, side).wait_send()
                send_half(k, side).wait_send()


def backward(dy, h1, A, H, G, U, WG, WU, WD, DGU, rows_d):
    tokens, d = dy.shape
    ff = WD.shape[1]
    dma = lambda *s: pltpu.SemaphoreType.DMA(s)
    like = lambda *s: jax.ShapeDtypeStruct(s, BF16)
    kinds = ((rows_d, d), (ff, 128), (ff, 128))
    one = [like(2, *s) for s in kinds]
    outs = pl.pallas_call(
        bwd_kernel,
        name="backward",
        in_specs=[ANY] * 10,
        out_specs=[ANY] * 18,
        out_shape=one + [like(2, tokens, ff), like(2, ff, d), like(2, 2, d // 128, ff, 128)]
        + [like(2, 4, *s) for s in kinds] + one * 3,
        scratch_shapes=[
            pltpu.VMEM((tokens, d), BF16), pltpu.VMEM((tokens, d), BF16), pltpu.VMEM((ff, d), BF16),
            pltpu.VMEM((d, ff), BF16), pltpu.VMEM((d, ff), BF16),
            pltpu.VMEM((9, rows_d, d), BF16), pltpu.VMEM((9, ff, 128), BF16),
            dma(8), dma(2, 8), dma(2), *[dma(8, 4)] * 2, *[dma(8, 2)] * 4,
        ],
        compiler_params=pltpu.CompilerParams(collective_id=1, has_side_effects=True, vmem_limit_bytes=64 * MB - 64 * 1024),
        cost_estimate=pl.CostEstimate(flops=20 * tokens * d * ff, bytes_accessed=200 * MB, transcendentals=0),
    )(dy, h1, A, H, G, U, WG, WU, WD, DGU)
    return outs[:3]


def optimizer(weights, m, v, grads):
    layers, rows, ff = weights[0].shape
    rows_d, d = weights[2].shape[1:]
    parts = 5
    wide = pl.BlockSpec((None, rows, ff // parts), lambda l, i: (l, 0, i))
    tall = pl.BlockSpec((None, ff // parts, rows), lambda l, i: (l, i, 0))
    flat = pl.BlockSpec((None, rows_d // parts, d), lambda l, i: (l, i, 0))

    def body(*refs):
        w, m, v, g = (refs[3 * n : 3 * n + 3] for n in range(4))
        for n in range(3):
            grad = g[n][...].astype(F32)
            new = adamw(w[n][...].astype(F32), m[n][...], v[n][...], grad if n == 2 else grad.T)
            for k in range(3):
                refs[12 + 3 * k + n][...] = new[k]

    three = [wide, wide, flat]
    return pl.pallas_call(
        body,
        name="optimizer",
        grid=(layers, parts),
        in_specs=three * 3 + [tall, tall, flat],
        out_specs=three * 3,
        out_shape=[jax.ShapeDtypeStruct(w.shape, t) for t in (BF16, F32, F32) for w in weights],
        compiler_params=pltpu.CompilerParams(vmem_limit_bytes=48 * MB),
    )(*weights, *m, *v, *grads)


def solution(mesh):
    def step(x, dy, *arrays):
        weights, m, v = (arrays[i : i + 3] for i in (0, 3, 6))
        x, dy = x[0], dy[0]
        WG, WU, WD, G, U, H, A, h1, DGU = forward(x, dy, *weights)
        grads = backward(dy, h1, A, H, G, U, WG, WU, WD, DGU, weights[2].shape[1])
        gd, gg, gu = grads
        return tuple(optimizer(weights, m, v, (gg, gu, gd)))

    states, cut = P(("rep", "dp"), None, None), P(None, "dp", None)
    return jax.shard_map(
        step,
        mesh=mesh,
        in_specs=(states, states) + (cut,) * 9,
        out_specs=(P("rep", "dp", None),) * 9,
        check_vma=False,
    )
```

```python
import re

import jax
import jax.numpy as jnp
from jax import lax
from jax.experimental import pallas as pl
from jax.experimental.pallas import tpu as pltpu
from jax.sharding import PartitionSpec as P

MESH = pl.DeviceIdType.MESH
F32, BF16 = jnp.float32, jnp.bfloat16
ANY = pl.BlockSpec(memory_space=pl.ANY)
BM = 512
MB = 2**20


def dot(a, b, ca=1, cb=0):
    return lax.dot_general(a, b, (((ca,), (cb,)), ((), ())), preferred_element_type=F32)


def normed(wide):
    scale = lax.rsqrt(jnp.mean(wide * wide, -1, keepdims=True) + 1e-6)
    return (wide * scale).astype(BF16)


def by_gate(gate, up, dh):
    sig = 0.5 * jnp.tanh(0.5 * gate) + 0.5
    silu = gate * sig
    return silu, (dh * up * (sig + silu * (1 - sig))).astype(BF16), (dh * silu).astype(BF16)


def plan(text):
    steps = {}
    for step, act, number in re.findall(r"(\d*)([A-Za-z])(\d+)", text):
        steps.setdefault(int(step or "0"), []).append((act, int(number)))
    return steps


def thirds(n, unit):
    tiles = n // unit
    side = tiles // 3
    return side * unit, (tiles - 2 * side) * unit, side * unit


def cuts(n):
    k = max(1, n // 512)
    return [(512 * j, 512 if j < k - 1 else n - 512 * j) for j in range(k)]


def fwd_kernel(
    x_ref, dy_ref, wg_ref, wu_ref, wd_ref,
    WG, WU, WD, G, U, H, A, h1_ref, DGU,
    sg, su, sd, a_v, x_v, hid_v, bg, bu, wd_v, st_g, st_u, st_d,
    io, ld, out_s, loc, own_s, own_r, rx_s, rx_r, dd_s, dd_r, pp_s, pp_r, pd_s, pd_r,
):
    tokens, d = x_v.shape
    steps = tokens // BM
    rep, me = lax.axis_index("rep"), lax.axis_index("dp")
    chips = 4
    xx, c = me // 2, lax.rem(me, 2)
    right = lax.rem(xx + 1, chips) * 2 + c
    left = lax.rem(xx + chips - 1, chips) * 2 + c
    opp = lax.rem(xx + 2, chips) * 2 + c
    core = xx * 2 + (1 - c)
    p = lax.rem(rep, 2)
    pair = rep + 1 - 2 * p
    to_right, to_left, to_core = {"dp": right}, {"dp": left}, {"dp": core}
    to_pair = {"rep": pair}
    others = [lax.rem(xx + k, chips) * 2 + (1 - c) for k in (chips - 1, 1, 2, 2)]
    mine = [left, right, opp, opp]

    shards = {"g": sg, "u": su, "d": sd}
    inputs = {"g": wg_ref, "u": wu_ref, "d": wd_ref}
    whole = {"g": WG, "u": WU, "d": WD}
    order = [(kind, 0) for kind in "gud"] + [(kind, 1) for kind in "dgu"]
    number = {key: k for k, key in enumerate(order)}
    ring = [(name[0], int(name[1]), int(name[2])) for name in "g00 u00 g01 u01".split() + "d00 d01 d10 d11".split() + "g10 u10 g11 u11".split()]

    def extent(kind, pos):
        rows, cols = shards[kind].shape[1:]
        n, unit = (rows, 16) if kind == "d" else (cols, 128)
        w = thirds(n, unit)
        far = n - w[2]
        off = (p * far, w[0], (1 - p) * far)[pos]
        if pos != 1:
            off = pl.multiple_of(off, unit)
        return (off, w[pos], 0, cols) if kind == "d" else (0, rows, off, w[pos])

    def region(ref, kind, layer, pos, base, half=None):
        r0, rows, c0, cols = extent(kind, pos)
        if half is not None:
            first = (rows // 2 + 15) // 16 * 16
            r0, rows = (r0, first) if half == 0 else (r0 + first, rows - first)
        start = r0 + base
        if not isinstance(start, int):
            start = pl.multiple_of(start, 16)
        return ref.at[layer, pl.ds(start, rows), pl.ds(c0, cols)]

    def place(kind, layer, pos, shard, half=None):
        return region(whole[kind], kind, layer, pos, shard * shards[kind].shape[1], half)

    def remote(src, dst, ss, rs, to):
        return pltpu.make_async_remote_copy(src_ref=src, dst_ref=dst, send_sem=ss, recv_sem=rs, device_id=to, device_id_type=MESH)

    def got(dst, ss, rs):
        remote(dst, dst, ss, rs, to_core).wait_recv()

    HALF = (None, None, 0, 1)

    def send_ring(k, j):
        kind, layer, pos = ring[k]
        if j < 2:
            src = region(shards[kind], kind, layer, pos, 0)
            dst = place(kind, layer, pos, me)
            return remote(src, dst, rx_s.at[k, j], rx_r.at[k, j], (to_right, to_left)[j])
        shard = (left, right)[j - 2]
        at = place(kind, layer, pos, shard, j - 2)
        return remote(at, at, rx_s.at[k, j], rx_r.at[k, j], (to_right, to_left)[j - 2])

    def recv_ring(k, j):
        kind, layer, pos = ring[k]
        got(place(kind, layer, pos, mine[j], HALF[j]), rx_s.at[k, j], rx_r.at[k, j])

    def send_core(k, j):
        kind, layer, pos = ring[k]
        at = place(kind, layer, pos, mine[j], HALF[j])
        return remote(at, at, dd_s.at[k, j], dd_r.at[k, j], to_core)

    def recv_core(k, j):
        kind, layer, pos = ring[k]
        got(place(kind, layer, pos, others[j], HALF[j]), dd_s.at[k, j], dd_r.at[k, j])

    def send_pair(k, j):
        kind, layer, pos = ring[k]
        q = number[kind, layer]
        at = place(kind, layer, pos, mine[j], HALF[j])
        return remote(at, at, pp_s.at[q, j], pp_r.at[q, j], to_pair)

    def recv_pair(q, j):
        kind, layer = order[q]
        got(place(kind, layer, 2, mine[j], HALF[j]), pp_s.at[q, j], pp_r.at[q, j])

    def send_pair_core(q, j):
        kind, layer = order[q]
        at = place(kind, layer, 2, mine[j], HALF[j])
        return remote(at, at, pd_s.at[q, j], pd_r.at[q, j], to_core)

    def recv_pair_core(q, j):
        kind, layer = order[q]
        got(place(kind, layer, 2, others[j], HALF[j]), pd_s.at[q, j], pd_r.at[q, j])

    def slot_of(kind, layer, shard):
        rows = shards[kind].shape[1]
        return whole[kind].at[layer, pl.ds(pl.multiple_of(shard * rows, 16), rows), :]

    def send_own(q):
        kind, layer = order[q]
        return remote(shards[kind].at[layer], slot_of(kind, layer, me), own_s.at[q], own_r.at[q], to_core)

    def recv_own(q):
        kind, layer = order[q]
        got(slot_of(kind, layer, core), own_s.at[q], own_r.at[q])

    def keep_own(q):
        kind, layer = order[q]
        return pltpu.make_async_copy(shards[kind].at[layer], slot_of(kind, layer, me), loc.at[q])

    def I(k):
        for j in range(2):
            send_ring(k, j).start()

    def onward(k, j):
        send_core(k, j).start()
        if ring[k][2] == 0:
            send_pair(k, j).start()

    def Fw(k):
        for j in range(2):
            recv_ring(k, j)
            send_ring(k, 2 + j).start()
            onward(k, j)

    def Gw(k):
        for j in (2, 3):
            recv_ring(k, j)
            onward(k, j)

    def Hw(q):
        for j in range(4):
            recv_pair(q, j)
            send_pair_core(q, j).start()

    def whole_piece(kind, layer, pos):
        if pos == 2:
            for j in range(4):
                recv_pair_core(number[kind, layer], j)
        else:
            for j in range(4):
                recv_core(ring.index((kind, layer, pos)), j)

    def head():
        for act, n in plan("F0,I2,F1,I3,G0,F2,I4,G1")[0]:
            {"I": I, "F": Fw, "G": Gw}[act](n)

    first = [pltpu.make_async_copy(inputs[kind], shards[kind], io.at[n]) for n, kind in enumerate("gud")]
    for copy in first:
        copy.start()
    load_x = pltpu.make_async_copy(x_ref, x_v, io.at[3])
    load_x.start()
    barrier = pltpu.get_barrier_semaphore()
    for to in (to_right, to_left, to_core, to_pair):
        pl.semaphore_signal(barrier, inc=1, device_id=to, device_id_type=MESH)
    pl.semaphore_wait(barrier, 4)
    for copy in first:
        copy.wait()
    I(0)
    I(1)
    for q in range(2):
        send_own(q).start()
        keep_own(q).start()
    load_x.wait()

    @pl.loop(0, steps)
    def _(m):
        rows = pl.ds(pl.multiple_of(m * BM, BM), BM)
        a_v[rows, :] = normed(x_v[rows, :].astype(F32))

    keep_a = [pltpu.make_async_copy(a_v, A.at[layer], io.at[4 + layer]) for layer in range(2)]
    keep_a[0].start()
    head()
    for q in range(2, 6):
        send_own(q).start()
        keep_own(q).start()
    for q in range(2):
        keep_own(q).wait()
        recv_own(q)

    widths = thirds(wg_ref.shape[2], 128)
    starts = (0, widths[0], widths[0] + widths[1])

    def load_weights(layer, pos):
        _, _, c0, cols = extent("g", pos)
        slot = pos % 2
        return [
            pltpu.make_async_copy(w.at[layer, :, pl.ds(c0, cols)], b.at[slot, :, pl.ds(0, cols)], ld.at[slot, n])
            for n, (w, b) in enumerate(((WG, bg), (WU, bu)))
        ]

    def store_out(layer, pos, m):
        _, _, c0, cols = extent("g", pos)
        slot = lax.rem(m, 2)
        rows = pl.ds(pl.multiple_of(m * BM, BM), BM)
        if layer:
            copies = [
                pltpu.make_async_copy(st_d.at[slot, n, :, pl.ds(0, cols)], DGU.at[n, rows, pl.ds(c0, cols)], out_s.at[slot, n])
                for n in range(2)
            ]
        else:
            copies = [
                pltpu.make_async_copy(st.at[slot, :, pl.ds(0, cols)], out.at[rows, pl.ds(c0, cols)], out_s.at[slot, n])
                for n, (st, out) in enumerate(((st_g, G), (st_u, U)))
            ]
        return copies + [
            pltpu.make_async_copy(hid_v.at[rows, pl.ds(starts[pos], cols)], H.at[layer, rows, pl.ds(c0, cols)], out_s.at[slot, 2]),
        ]

    def gate_up(layer, pos, acts):
        cols = widths[pos]
        slot = pos % 2
        for copy in load_weights(layer, pos):
            copy.wait()

        @pl.loop(0, steps)
        def _(m):
            at_step(m, acts)
            rows = pl.ds(pl.multiple_of(m * BM, BM), BM)
            back = lax.rem(m, 2)

            @pl.when(m >= 2)
            def _():
                for copy in store_out(layer, pos, m - 2):
                    copy.wait()

            if pos:

                @pl.when(m < 2)
                def _():
                    for copy in store_out(layer, pos - 1, m + steps - 2):
                        copy.wait()

            a = a_v[rows, :]
            for c0, w in cuts(cols):
                gate = dot(a, bg[slot, :, c0 : c0 + w])
                up = dot(a, bu[slot, :, c0 : c0 + w])
                at = starts[pos] + c0
                if layer:
                    dh = dot(x_v[rows, :], wd_v[at : at + w, :], 1, 1).astype(BF16).astype(F32)
                    silu, dg, du = by_gate(gate, up, dh)
                    st_d[back, 0, :, c0 : c0 + w] = dg
                    st_d[back, 1, :, c0 : c0 + w] = du
                else:
                    st_g[back, :, c0 : c0 + w] = gate
                    st_u[back, :, c0 : c0 + w] = up
                    silu = gate * (0.5 * jnp.tanh(0.5 * gate) + 0.5)
                hid_v[rows, at : at + w] = (silu * up).astype(BF16)
            for copy in store_out(layer, pos, m):
                copy.start()

        if pos == 2:
            for m in (steps - 2, steps - 1):
                for copy in store_out(layer, pos, m):
                    copy.wait()

    def ready(layer, pos):
        def act():
            for kind in "gu":
                whole_piece(kind, layer, pos)
            for copy in load_weights(layer, pos):
                copy.start()

        return act

    def then(acts):
        for todo in plan(acts).values():
            for act, n in todo:
                moves[act](n)

    def R(n):
        ready(n // 3, n % 3)()

    def O(_):
        own_1()

    moves = {"I": I, "F": Fw, "G": Gw, "H": Hw, "R": R, "O": O}

    def at_step(m, acts):
        for when, todo in plan(acts).items():

            @pl.when(m == when)
            def _():
                for act, n in todo:
                    moves[act](n)

    def load_down(layer):
        copies = []
        for n in range(3):
            _, _, c0, cols = extent("g", n)
            copies.append(pltpu.make_async_copy(WD.at[layer, pl.ds(c0, cols), :], wd_v.at[pl.ds(starts[n], cols), :], io.at[6 + n]))
        return copies

    def start_down(layer):
        q = number["d", layer]
        keep_own(q).wait()
        recv_own(q)
        for pos in range(3):
            whole_piece("d", layer, pos)
        for copy in load_down(layer):
            copy.start()

    def own_1():
        for q in (4, 5):
            keep_own(q).wait()
            recv_own(q)

    then("R0")
    gate_up(0, 0, "2F3,2I5,3G2")
    then("F4,I6,G3,R1")
    gate_up(0, 1, "1H0,1F5,1I7,3G4,3H1,3R2")
    gate_up(0, 2, "0F6,0I8,1G5,2H2,3F7,3I9")
    start_down(0)
    keep_a[0].wait()
    for copy in load_down(0):
        copy.wait()
    half = BM // 2

    @pl.loop(0, 2 * steps)
    def _(m):
        at_step(m, "0G6,3F8,5G7,7H3,7O0")
        rows = pl.ds(pl.multiple_of(m * half, half), half)
        h = x_v[rows, :] + dot(hid_v[rows, :], wd_v[...]).astype(BF16)
        x_v[rows, :] = h
        a_v[rows, :] = normed(h.astype(F32))

    keep_h = pltpu.make_async_copy(x_v, h1_ref, io.at[9])
    keep_h.start()
    keep_a[1].start()
    start_down(1)
    then("F9,I10,I11,G8")
    keep_h.wait()
    load_dy = pltpu.make_async_copy(dy_ref, x_v, io.at[3])
    load_dy.start()
    then("G9,R3")
    for copy in load_down(1):
        copy.wait()
    load_dy.wait()
    gate_up(1, 0, "2F10,3F11,3G10")
    then("G11,R4")
    gate_up(1, 1, "1H4,1H5,3R5")
    gate_up(1, 2, "")
    keep_a[1].wait()
    for k in range(len(ring)):
        for j in range(4):
            send_ring(k, j).wait_send()
            send_core(k, j).wait_send()
            if ring[k][2] == 0:
                send_pair(k, j).wait_send()
    for q in range(len(order)):
        send_own(q).wait_send()
        for j in range(4):
            send_pair_core(q, j).wait_send()


def forward(x, dy, wg, wu, wd):
    tokens, d = x.shape
    layers, _, ff = wg.shape
    dma = lambda *s: pltpu.SemaphoreType.DMA(s)
    big = max(thirds(ff, 128))
    like = lambda s, t=BF16: jax.ShapeDtypeStruct(s, t)
    return pl.pallas_call(
        fwd_kernel,
        name="forward",
        in_specs=[ANY] * 5,
        out_specs=[ANY] * 9,
        out_shape=[
            like((layers, d, ff)), like((layers, d, ff)), like((layers, ff, d)),
            like((tokens, ff), F32), like((tokens, ff), F32), like((layers, tokens, ff)),
            like((layers, tokens, d)), like((tokens, d)), like((2, tokens, ff)),
        ],
        scratch_shapes=[
            pltpu.VMEM(wg.shape, BF16), pltpu.VMEM(wu.shape, BF16), pltpu.VMEM(wd.shape, BF16),
            pltpu.VMEM((tokens, d), BF16), pltpu.VMEM((tokens, d), BF16), pltpu.VMEM((tokens, ff), BF16),
            pltpu.VMEM((2, d, big), BF16), pltpu.VMEM((2, d, big), BF16), pltpu.VMEM((ff, d), BF16),
            pltpu.VMEM((2, BM, big), F32), pltpu.VMEM((2, BM, big), F32), pltpu.VMEM((2, 2, BM, big), BF16),
            dma(10), dma(2, 2), dma(2, 3), *[dma(6)] * 3, *[dma(12, 4)] * 4, *[dma(6, 4)] * 4,
        ],
        compiler_params=pltpu.CompilerParams(collective_id=0, has_side_effects=True, vmem_limit_bytes=64 * MB - 64 * 1024),
        cost_estimate=pl.CostEstimate(flops=10 * tokens * d * ff, bytes_accessed=200 * MB, transcendentals=0),
    )(x, dy, wg, wu, wd)


def adamw(w, m, v, g):
    m = 0.9 * m + 0.1 * g
    v = 0.95 * v + 0.05 * g * g
    step = m * lax.rsqrt(v + 1e-8) + 0.1 * w
    return (w - 0.02 * step).astype(jnp.bfloat16), m, v


def bwd_kernel(
    dy_ref, h_ref, A, H, G, U, WG, WU, WD, DGU,
    gd, gg, gu, DGU0, Dd, Dgu, Pd, Pg, Pu, Hd, Hg, Hu, Ld, Lg, Lu, Rd, Rg, Ru,
    v0, v1, wd_v, wg_v, wu_v, big_d, big_g,
    io, ld, ost, ds, dr, hs, hr, fs, fr,
):
    tokens, d = v0.shape
    ff = wd_v.shape[0]
    me = lax.axis_index("dp")
    chips = 4
    xx, c = me // 2, lax.rem(me, 2)
    ahead = [lax.rem(xx + k, chips) for k in range(chips)]
    to_right, to_left = {"dp": ahead[1] * 2 + c}, {"dp": ahead[3] * 2 + c}
    to_core = {"dp": xx * 2 + (1 - c)}

    others = {"d": Pd, "g": Pg, "u": Pu}
    halves = {"d": Hd, "g": Hg, "u": Hu}
    lefts = {"d": Ld, "g": Lg, "u": Lu}
    rights = {"d": Rd, "g": Rg, "u": Ru}
    outs = {"d": gd, "g": gg, "u": gu}
    split = ff // 640 // 2 * 640
    rows_d = gd.shape[1]
    tasks = [("d", 1, 0, rows_d), ("g", 1, 0, ff), ("u", 1, 0, ff), ("d", 0, 0, rows_d)]
    tasks += [(kind, 0, r0, n) for kind in "gu" for r0, n in ((0, split), (split, ff - split))]
    before = []
    for k, (kind, *_) in enumerate(tasks):
        same = [q for q in range(k) if (tasks[q][0] == "d") == (kind == "d")]
        before.append(same[-1] if same else None)

    def remote(src, dst, ss, rs, to):
        return pltpu.make_async_remote_copy(src_ref=src, dst_ref=dst, send_sem=ss, recv_sem=rs, device_id=to, device_id_type=MESH)

    def own(k, chip, core):
        kind, layer, r0, n = tasks[k]
        shard = chip * 2 + core
        if kind == "d":
            return Dd.at[layer, pl.ds(pl.multiple_of(shard * rows_d, 16), n), :]
        return Dgu.at[layer, "gu".index(kind), shard, pl.ds(r0, n), :]

    def other(k, chip):
        kind, layer, r0, n = tasks[k]
        return others[kind].at[layer, chip, pl.ds(r0, n), :]

    def at(refs, k, half=None):
        kind, layer, r0, n = tasks[k]
        a, b = cut(n, half)
        return refs[kind].at[layer, pl.ds(r0 + a, b), :]

    def cut(n, half):
        if half is None:
            return 0, n
        first = (n // 2 + 15) // 16 * 16
        return (0, first) if half == 0 else (first, n - first)

    def buf(k, which, half=None):
        kind, _, _, n = tasks[k]
        a, b = cut(n, half)
        return (big_d if kind == "d" else big_g).at[which, pl.ds(a, b), :]

    def load(k, src, which):
        return pltpu.make_async_copy(src, buf(k, which), ld.at[0 if tasks[k][0] == "d" else 1, which])

    def add(k, out, terms, half=None):
        ref = big_d if tasks[k][0] == "d" else big_g
        a, n = cut(tasks[k][3], half)
        step = 64 if tasks[k][0] == "d" else 320

        def some(rows):
            total = ref[terms[0], rows, :].astype(F32)
            for t in terms[1:]:
                total += ref[t, rows, :].astype(F32)
            ref[out, rows, :] = total.astype(BF16)

        @pl.loop(0, n // step)
        def _(i):
            some(pl.ds(pl.multiple_of(a + i * step, 16), step))

        if n % step:
            some(pl.ds(a + n // step * step, n % step))

    def to_other(k, chip):
        return remote(own(k, chip, 1 - c), other(k, chip), ds.at[k, chip], dr.at[k, chip], to_core)

    def send_half(k, half):
        return remote(buf(k, 8, half), at(halves, k, half), hs.at[k, half], hr.at[k, half], (to_right, to_left)[half])

    def send_full(k, side):
        return remote(buf(k, 5 + side), at((lefts, rights)[side], k), fs.at[k, side], fr.at[k, side], (to_right, to_left)[side])

    def A_(k):
        for chip in range(chips):
            to_other(k, chip).start()

    def loads(k, what):
        two = lambda chip: [load(k, own(k, ahead[chip], c), 0), load(k, other(k, ahead[chip]), 1)]
        if what == "B":
            return two(2)
        if what == "C":
            return two(1) + [load(k, own(k, ahead[3], c), 2), load(k, other(k, ahead[3]), 3), load(k, at(halves, k), 4)]
        return two(0) + [load(k, at(lefts, k), 2), load(k, at(rights, k), 3)]

    def B0(k):
        for chip in range(chips):
            to_other(k, chip).wait_recv()
        for copy in loads(k, "B"):
            copy.start()

    def B1(k):
        for copy in loads(k, "B"):
            copy.wait()
        if before[k] is not None:
            for half in range(2):
                send_half(before[k], half).wait_send()
        add(k, 8, (0, 1))
        for half in range(2):
            send_half(k, half).start()

    def C0(k):
        for half in range(2):
            send_half(k, half).wait_recv()
        for copy in loads(k, "C"):
            copy.start()

    def C1(k):
        for copy in loads(k, "C"):
            copy.wait()
        if before[k] is not None:
            for side in range(2):
                send_full(before[k], side).wait_send()
        add(k, 5, (0, 1, 4), 0)
        add(k, 5, (0, 1), 1)
        send_full(k, 0).start()
        add(k, 6, (2, 3), 0)
        add(k, 6, (2, 3, 4), 1)
        send_full(k, 1).start()

    def result(k):
        return pltpu.make_async_copy(buf(k, 7), at(outs, k), ost.at[0 if tasks[k][0] == "d" else 1])

    def D0(k):
        for side in range(2):
            send_full(k, side).wait_recv()
        for copy in loads(k, "D"):
            copy.start()

    def D1(k):
        for copy in loads(k, "D"):
            copy.wait()
        if before[k] is not None:
            result(before[k]).wait()
        add(k, 7, range(4))
        result(k).start()

    ACTS = {"A": A_, "b": B0, "B": B1, "c": C0, "C": C1, "d": D0, "D": D1}

    def perform(todo):
        for name, k in todo:
            ACTS[name](k)

    def run(acts):
        for todo in plan(acts).values():
            perform(todo)

    def acts_at(step, acts):
        for when, todo in plan(acts).items():

            @pl.when(step == when)
            def _():
                perform(todo)

    def pipe(body, grid, ins, outs_, acts):
        def inner(indices, *refs):
            acts_at(indices.local_index, acts)
            body(indices.index, *refs)

        pltpu.emit_pipeline(
            inner, grid=grid, in_specs=[s for s, _ in ins], out_specs=[s for s, _ in outs_], _explicit_indices=True
        )(*[r for _, r in ins], *[r for _, r in outs_])

    BF = 640
    tall = pl.BlockSpec((tokens, BF), lambda j: (0, j))

    def dw_down(layer, acts):
        def body(_, a_ref, o_ref):
            w = d // 2

            @pl.loop(0, 2)
            def _(n):
                cols = pl.ds(pl.multiple_of(n * w, 128), w)
                o_ref[:, cols] = dot(a_ref[...], v0[:, cols], 0, 0).astype(BF16)

        pipe(body, (ff // BF,), [(tall, H.at[layer])], [(pl.BlockSpec((BF, d), lambda j: (j, 0)), Dd.at[layer])], acts)

    def dw_up(src, layer, acts):
        n = ff // BF

        def body(_, a_ref, o_ref):
            for c0, w in cuts(d):
                part = dot(a_ref[...], v1[:, c0 : c0 + w], 0, 0).astype(BF16)
                for s in range(w // 128):
                    o_ref[c0 // 128 + s, :, :] = part[:, 128 * s : 128 * s + 128]

        a_spec = pl.BlockSpec((None, tokens, BF), lambda s: (s // n, 0, s % n))
        spec = pl.BlockSpec((None, d // 128, BF, 128), lambda s: (s // n, 0, s % n, 0))
        pipe(body, (2 * n,), [(a_spec, src)], [(spec, Dgu.at[layer])], acts)

    def gates(acts):
        bm = 512

        def body(indices, g_ref, u_ref, dg_ref):
            j, i = indices
            by = v0[pl.ds(pl.multiple_of(i * bm, bm), bm), :]
            for c0, w in ((0, 256), (256, 384)):
                wd = wd_v[pl.ds(pl.multiple_of(j * BF + c0, 128), w), :]
                dh = dot(by, wd, 1, 1).astype(BF16).astype(F32)
                _, dg, du = by_gate(g_ref[:, c0 : c0 + w], u_ref[:, c0 : c0 + w], dh)
                dg_ref[0, :, c0 : c0 + w] = dg
                dg_ref[1, :, c0 : c0 + w] = du

        spec = pl.BlockSpec((bm, BF), lambda j, i: (i, j), pipeline_mode=pl.Buffered(3))
        out = pl.BlockSpec((2, bm, BF), lambda j, i: (0, i, j))
        pipe(body, (ff // BF, tokens // bm), [(spec, G), (spec, U)], [(out, DGU0)], acts)

    def states(acts):
        bm = 256

        def body(indices, dgu_ref, hh_ref):
            rows = pl.ds(pl.multiple_of(indices[0] * bm, bm), bm)
            da = dot(dgu_ref[0], wg_v[...], 1, 1).astype(BF16).astype(F32) + dot(dgu_ref[1], wu_v[...], 1, 1).astype(BF16).astype(F32)
            da = da.astype(BF16).astype(F32)
            wide = hh_ref[...].astype(F32)
            scale = lax.rsqrt(jnp.mean(wide * wide, -1, keepdims=True) + 1e-6)
            along = jnp.mean(da * wide, -1, keepdims=True)
            by = da * scale - wide * (scale * scale * scale * along)
            v0[rows, :] = v0[rows, :] + by.astype(BF16)

        spec = pl.BlockSpec((2, bm, ff), lambda i: (0, i, 0))
        pipe(body, (tokens // bm,), [(spec, DGU), (pl.BlockSpec((bm, d), lambda i: (i, 0)), h_ref)], [], acts)

    barrier = pltpu.get_barrier_semaphore()
    for to in (to_right, to_left, to_core):
        pl.semaphore_signal(barrier, inc=1, device_id=to, device_id_type=MESH)
    into = lambda src, dst, n: pltpu.make_async_copy(src, dst, io.at[n])
    c_dy, c_a1 = into(dy_ref, v0, 0), into(A.at[1], v1, 1)
    c_wg, c_wu = into(WG.at[1], wg_v, 3), into(WU.at[1], wu_v, 4)
    c_a0, c_wd0 = into(A.at[0], v1, 5), into(WD.at[0], wd_v, 6)
    c_dy.start()
    c_a1.start()
    pl.semaphore_wait(barrier, 3)
    c_dy.wait()
    dw_down(1, "")
    run("A0")
    c_a1.wait()
    c_wg.start()
    c_wu.start()
    c_wd0.start()
    dw_up(DGU, 1, "2b0,3B0,7A1,7c0,8C0")
    run("A2,b1,B1")
    c_a0.start()
    c_wg.wait()
    c_wu.wait()
    states("2b2,3B2,4d0,5D0,6c1,7C1")
    dw_down(0, "0c2,1C2,4d1")
    run("A3,D1")
    c_wd0.wait()
    c_a0.wait()
    gates("5b3,6B3,9d2,10D2,15c3,16C3")
    dw_up(
        DGU0, 0,
        "4A4,4d3,5D3,6b4,7B4,7A5,9b5",
    )
    run("A6,A7,B5,c4,C4,b6,B6,c5,C5,b7,B7,d4,D4")
    run("c6,C6,c7,C7,d5,D5,d6,D6,d7,D7")
    for k in range(len(tasks)):
        for chip in range(chips):
            to_other(k, chip).wait_send()
        if k not in before:
            result(k).wait()
            for side in range(2):
                send_full(k, side).wait_send()
                send_half(k, side).wait_send()


def backward(dy, h1, A, H, G, U, WG, WU, WD, DGU, rows_d):
    tokens, d = dy.shape
    ff = WD.shape[1]
    dma = lambda *s: pltpu.SemaphoreType.DMA(s)
    like = lambda *s: jax.ShapeDtypeStruct(s, BF16)
    kinds = ((rows_d, d), (ff, 128), (ff, 128))
    one = [like(2, *s) for s in kinds]
    outs = pl.pallas_call(
        bwd_kernel,
        name="backward",
        in_specs=[ANY] * 10,
        out_specs=[ANY] * 18,
        out_shape=one + [like(2, tokens, ff), like(2, ff, d), like(2, 2, d // 128, ff, 128)]
        + [like(2, 4, *s) for s in kinds] + one * 3,
        scratch_shapes=[
            pltpu.VMEM((tokens, d), BF16), pltpu.VMEM((tokens, d), BF16), pltpu.VMEM((ff, d), BF16),
            pltpu.VMEM((d, ff), BF16), pltpu.VMEM((d, ff), BF16),
            pltpu.VMEM((9, rows_d, d), BF16), pltpu.VMEM((9, ff, 128), BF16),
            dma(8), dma(2, 8), dma(2), *[dma(8, 4)] * 2, *[dma(8, 2)] * 4,
        ],
        compiler_params=pltpu.CompilerParams(collective_id=1, has_side_effects=True, vmem_limit_bytes=64 * MB - 64 * 1024),
        cost_estimate=pl.CostEstimate(flops=20 * tokens * d * ff, bytes_accessed=200 * MB, transcendentals=0),
    )(dy, h1, A, H, G, U, WG, WU, WD, DGU)
    return outs[:3]


def optimizer(weights, m, v, grads):
    layers, rows, ff = weights[0].shape
    rows_d, d = weights[2].shape[1:]
    parts = 5
    wide = pl.BlockSpec((None, rows, ff // parts), lambda l, i: (l, 0, i))
    tall = pl.BlockSpec((None, ff // parts, rows), lambda l, i: (l, i, 0))
    flat = pl.BlockSpec((None, rows_d // parts, d), lambda l, i: (l, i, 0))

    def body(*refs):
        w, m, v, g = (refs[3 * n : 3 * n + 3] for n in range(4))
        for n in range(3):
            grad = g[n][...].astype(F32)
            new = adamw(w[n][...].astype(F32), m[n][...], v[n][...], grad if n == 2 else grad.T)
            for k in range(3):
                refs[12 + 3 * k + n][...] = new[k]

    three = [wide, wide, flat]
    return pl.pallas_call(
        body,
        name="optimizer",
        grid=(layers, parts),
        in_specs=three * 3 + [tall, tall, flat],
        out_specs=three * 3,
        out_shape=[jax.ShapeDtypeStruct(w.shape, t) for t in (BF16, F32, F32) for w in weights],
        compiler_params=pltpu.CompilerParams(vmem_limit_bytes=48 * MB),
    )(*weights, *m, *v, *grads)


def solution(mesh):
    def step(x, dy, *arrays):
        weights, m, v = (arrays[i : i + 3] for i in (0, 3, 6))
        x, dy = x[0], dy[0]
        WG, WU, WD, G, U, H, A, h1, DGU = forward(x, dy, *weights)
        grads = backward(dy, h1, A, H, G, U, WG, WU, WD, DGU, weights[2].shape[1])
        gd, gg, gu = grads
        return tuple(optimizer(weights, m, v, (gg, gu, gd)))

    states, cut = P(("rep", "dp"), None, None), P(None, "dp", None)
    return jax.shard_map(
        step,
        mesh=mesh,
        in_specs=(states, states) + (cut,) * 9,
        out_specs=(P("rep", "dp", None),) * 9,
        check_vma=False,
    )
```
